32 devices in a mesh: pair: 8 (over z, y), aux: 4 (over x, core).
Axes of the slice: x: 2, y: 2, z: 4, core: 2. Of those that a mesh axis runs over, the one named last changes fastest.
Arguments:
- ints_ac: bfloat16 [192, 512, 4096], P(None, ('pair', 'aux')), may hold values from -0.375 to 0.375
- slot_pair: int32 [192], replicated, may hold values from 0 to 191, each once
- amplitudes: bfloat16 [192, 2, 4096], P(('pair', 'aux')), may hold values from -6 to 6
- ranks: int32 [192], P(('pair', 'aux')), may hold values from 16 to 64
- pair_occ: int32 [192, 2], P(('pair', 'aux')), may hold values from 0 to 47
- pno_energy: float32 [192, 64], P(('pair', 'aux')), may hold values from 0.2 to 3
- occ_energy: float32 [48], replicated, may hold values from -2 to -0.3
Outputs:
- ext_residual: float32 [192, 2, 4096], P(('pair', 'aux'))
- new_amplitudes: bfloat16 [192, 2, 4096], P(('pair', 'aux'))
The draws below stay inside these ranges and needn't reach their ends.
Inputs may be any that keep to these rules, and one draw needn't show every extreme that they name: `slot_pair`: a permutation of the pairs. Entries a >= ranks[s] of a slot's blocks are padding.
All inputs are finite; a program needn't handle non-finite values.
Results may differ from the reference program's by a relative error of at most 0.0039.
Values may be sent and summed in bfloat16 or wider, within the bound.
A program may use at most 128 MiB of HBM per device.

```python
import jax
import jax.numpy as jnp
from jax import lax

RANK = 64
NAUX = 512
NOCC = 48
PAIRS = 192


def plant(entries, own_key, low, largest):
    longest = entries.shape.index(max(entries.shape))
    spots = []
    for shift in (0, 1):
        where = [jax.random.randint(jax.random.fold_in(own_key, axis), (), 0, length) for axis, length in enumerate(entries.shape)]
        where[longest] = (where[longest] + shift) % entries.shape[longest]
        spots.append(tuple(where))
    return entries.at[spots[0]].set(low).at[spots[1]].set(largest)


def block_scale(rng, dims, pieces, low, top_value):
    level, own = 1.0, jax.random.fold_in(rng, 6)
    for dim, blocks in pieces:
        heights = jnp.exp(jax.random.uniform(jax.random.fold_in(own, dim), (blocks,), jnp.float32, low / len(pieces), top_value / len(pieces)))
        level = level * jnp.repeat(heights, dims[dim] // blocks).reshape([-1 if axis == dim else 1 for axis in range(len(dims))])
    return level


def normal_values(stream_key, extent, spread, most, cuts=(), kind=jnp.bfloat16):
    factor_of = block_scale(stream_key, extent, cuts, -0.22, 0.18) if cuts else 1.0
    array = jax.random.normal(stream_key, extent, jnp.float32) * spread * factor_of
    return jnp.minimum(jnp.maximum(array, -most), most).astype(kind)


def setup_inputs(seed: int = 0) -> dict:
    key_list = jax.random.split(jax.random.key(seed), 8)
    return {
        "ints_ac": normal_values(key_list[0], (PAIRS, NAUX, RANK * RANK), ((NAUX * RANK * RANK) ** -0.25), 0.375, ((1, 32),)),
        "slot_pair": jax.random.permutation(key_list[1], PAIRS).astype(jnp.int32),
        "amplitudes": normal_values(key_list[2], (PAIRS, 2, RANK * RANK), 1.0, 6.0, ((0, 32),)),
        "ranks": plant(jax.random.randint(key_list[3], (PAIRS,), RANK // 4, RANK + 1), jax.random.fold_in(key_list[3], 1), RANK // 4, RANK).astype(jnp.int32),
        "pair_occ": plant(jax.random.randint(key_list[4], (PAIRS, 2), 0, NOCC), jax.random.fold_in(key_list[4], 1), 0, NOCC - 1).astype(jnp.int32),
        "pno_energy": jnp.clip(0.2 + 2.8 * jax.random.uniform(key_list[5], (PAIRS, RANK), jnp.float32) ** block_scale(key_list[5], (PAIRS, RANK), ((0, 32),), -0.2, 0.2), 0.2, 3.0),
        "occ_energy": jnp.clip(jax.random.uniform(key_list[6], (NOCC,), jnp.float32, -2.0, -0.3), -2.0, -0.3),
    }


def reference(ints_ac, slot_pair, amplitudes, ranks, pair_occ, pno_energy, occ_energy):
    positions = jnp.arange(RANK, dtype=jnp.int32)
    masks = (positions[None, :] < ranks[:, None]).astype(jnp.float32)

    def one_slot(slot):
        pair_index = slot_pair[slot].astype(jnp.int32)
        block = lax.dynamic_index_in_dim(ints_ac, pair_index, 0, keepdims=False)
        amps = lax.dynamic_index_in_dim(amplitudes, slot, 0, keepdims=False)
        mask = lax.dynamic_index_in_dim(masks, slot, 0, keepdims=False)
        square = (mask[:, None] * mask[None, :]).reshape(RANK * RANK).astype(jnp.bfloat16)
        masked_b = (block * square).reshape(NAUX, RANK, RANK).astype(jnp.float32)
        masked_t = (amps * square).reshape(2, RANK, RANK).astype(jnp.float32)
        inner = jnp.einsum("pac,kcd->pakd", masked_b, masked_t).astype(jnp.bfloat16).astype(jnp.float32)
        result = jnp.einsum("pakd,pbd->kab", inner, masked_b)
        return result.reshape(2, RANK * RANK)

    ext_residual = lax.map(one_slot, jnp.arange(PAIRS, dtype=jnp.int32))
    occ_pair = occ_energy[pair_occ]
    denom = pno_energy[:, :, None] + pno_energy[:, None, :] - (occ_pair[:, 0] + occ_pair[:, 1])[:, None, None]
    square = masks[:, :, None] * masks[:, None, :]
    masked_t = amplitudes.astype(jnp.float32).reshape(PAIRS, 2, RANK, RANK) * square[:, None]
    updated = (masked_t - ext_residual.reshape(PAIRS, 2, RANK, RANK) / denom[:, None]) * square[:, None]
    new_amplitudes = updated.reshape(PAIRS, 2, RANK * RANK).astype(jnp.bfloat16)
    return ext_residual, new_amplitudes
```

```python
import jax
import jax.numpy as jnp
from jax import lax
from jax.experimental import pallas as pl
from jax.experimental.pallas import tpu as pltpu
from jax.sharding import PartitionSpec as P

GROUP = 8


def exchange_kernel(group, width, order_ref, *refs):
    blocks, amps_ref, out_ref, rows_ref = refs[:group], refs[group], refs[group + 1], refs[group + 2]
    lanes = 2 * width
    aux = blocks[0].shape[1]
    chunks = width * width // lanes
    half_t = lax.broadcasted_iota(jnp.int32, (width, lanes), 1) < width
    half_b = lax.broadcasted_iota(jnp.int32, (chunks, lanes), 1) < width
    for slot in range(group):
        block = blocks[slot]
        for chunk in range(chunks):
            rows_ref[slot, pl.ds(chunk * aux, aux), :] = block[
                0, :, pl.ds(chunk * lanes, lanes)
            ].astype(jnp.float32)
        pieces = []
        for pair in range(aux // 2):
            first = rows_ref[slot, pl.ds(2 * pair, chunks, stride=aux), :]
            second = rows_ref[slot, pl.ds(2 * pair + 1, chunks, stride=aux), :]
            even = jnp.where(half_b, first, pltpu.roll(second, width, 1))
            odd = jnp.where(half_b, pltpu.roll(first, width, 1), second)
            pieces.append(jnp.concatenate([even, odd], axis=0).astype(jnp.bfloat16))
        stacked = jnp.concatenate(pieces, axis=0)
        amps = amps_ref[slot].astype(jnp.float32)
        turned = pltpu.roll(amps, width, 1)
        none = jnp.zeros_like(amps)
        weights = jnp.concatenate(
            [
                jnp.concatenate([jnp.where(half_t, amps, none), jnp.where(half_t, none, turned)], axis=0),
                jnp.concatenate([jnp.where(half_t, turned, none), jnp.where(half_t, none, amps)], axis=0),
            ],
            axis=1,
        ).astype(jnp.bfloat16)
        inner = jnp.dot(stacked, weights, preferred_element_type=jnp.float32).astype(jnp.bfloat16)
        left = jnp.concatenate(pieces, axis=1)
        right = jnp.concatenate(
            [
                jnp.concatenate(
                    [
                        inner[pair * width : (pair + 1) * width, k * lanes : (k + 1) * lanes]
                        for pair in range(aux // 2)
                    ],
                    axis=1,
                )
                for k in range(2)
            ],
            axis=0,
        )
        out_ref[slot] = lax.dot_general(
            left, right, (((1,), (1,)), ((), ())), preferred_element_type=jnp.float32
        ).astype(out_ref.dtype)


def partials(ints_ac, slot_pair, amps):
    count, width, lanes = amps.shape
    aux = ints_ac.shape[1]
    group = max(g for g in range(1, GROUP + 1) if count % g == 0)

    def block_map(offset):
        return lambda step, order: (order[step * group + offset], 0, 0)

    return pl.pallas_call(
        lambda *refs: exchange_kernel(group, width, *refs),
        grid_spec=pltpu.PrefetchScalarGridSpec(
            num_scalar_prefetch=1,
            grid=(count // group,),
            in_specs=[
                pl.BlockSpec((1, aux, width * width), block_map(offset)) for offset in range(group)
            ]
            + [pl.BlockSpec((group, width, lanes), lambda step, order: (step, 0, 0))],
            out_specs=pl.BlockSpec((group, width, lanes), lambda step, order: (step, 0, 0)),
            scratch_shapes=[pltpu.VMEM((group, aux * width // 2, lanes), jnp.float32)],
        ),
        out_shape=jax.ShapeDtypeStruct((count, width, lanes), jnp.bfloat16),
        cost_estimate=pl.CostEstimate(
            flops=8 * count * aux * width**3,
            bytes_accessed=ints_ac.size * 2 + amps.size * 4,
            transcendentals=0,
        ),
        name="exchange",
    )(slot_pair, *([ints_ac] * group), amps)


def body(ints_ac, slot_pair, amplitudes, ranks, pair_occ, pno_energy, occ_energy):
    width = pno_energy.shape[1]
    local = amplitudes.shape[0]
    positions = jnp.arange(width, dtype=jnp.int32)
    masks = (positions[None, :] < ranks[:, None]).astype(jnp.float32)
    square = masks[:, :, None] * masks[:, None, :]
    masked_t = amplitudes.astype(jnp.float32).reshape(local, 2, width, width) * square[:, None]
    own = masked_t.astype(jnp.bfloat16).transpose(0, 2, 1, 3).reshape(local, width, 2 * width)
    every = lax.all_gather(own, ("pair", "aux"), axis=0, tiled=True)
    out = partials(ints_ac, slot_pair, every)
    parts = lax.all_to_all(out, ("pair", "aux"), 0, 0, tiled=True)
    parts = parts.reshape(-1, local, width, 2 * width)
    summed = parts.astype(jnp.float32).sum(axis=0)
    source = (positions % 2) * (width // 2) + positions // 2
    place = (positions[:, None] == source[None, :]).astype(jnp.float32)
    split = summed.reshape(local, width, 2, width)
    residual = jnp.einsum(
        "jykx,xa,yb->jkab", split, place, place, precision=lax.Precision.HIGHEST
    )
    residual = residual * square[:, None]
    onehot = (
        pair_occ[:, :, None] == jnp.arange(occ_energy.shape[0], dtype=jnp.int32)[None, None, :]
    ).astype(jnp.float32)
    occ_pair = jnp.einsum("jko,o->jk", onehot, occ_energy, precision=lax.Precision.HIGHEST)
    denom = (
        pno_energy[:, :, None]
        + pno_energy[:, None, :]
        - (occ_pair[:, 0] + occ_pair[:, 1])[:, None, None]
    )
    updated = (masked_t - residual / denom[:, None]) * square[:, None]
    return (
        residual.reshape(local, 2, width * width),
        updated.reshape(local, 2, width * width).astype(jnp.bfloat16),
    )


def solution(mesh):
    placed = (
        P(None, ("pair", "aux"), None),
        P(),
        P(("pair", "aux"), None, None),
        P(("pair", "aux")),
        P(("pair", "aux"), None),
        P(("pair", "aux"), None),
        P(),
    )
    return jax.shard_map(
        body,
        mesh=mesh,
        in_specs=placed,
        out_specs=(P(("pair", "aux"), None, None), P(("pair", "aux"), None, None)),
        check_vma=False,
    )
```
